32 devices in a mesh: clients: 8 (over y, x, core), shard: 4 (over z).
Axes of the slice: x: 2, y: 2, z: 4, core: 2. Of those that a mesh axis runs over, the one named last changes fastest.
Arguments:
- client_deltas: bfloat16 [64, 32, 3584], P(('clients', 'shard')), may hold values from -6 to 6
- variate_deltas: bfloat16 [64, 32, 3584], P(('clients', 'shard')), may hold values from -6 to 6
- params: float32 [32, 3584], P(('clients', 'shard')), may hold values from -1.5 to 1.5
- variate: float32 [32, 3584], P(('clients', 'shard')), may hold values from -1.5 to 1.5
- taking_part: int32 [64], P(('clients', 'shard')), may hold values from 0 to 1, as said below
- counts: int32 [64], P(('clients', 'shard')), may hold values from 32 to 285
Outputs:
- new_params: float32 [32, 3584], P(('clients', 'shard'))
- new_variate: float32 [32, 3584], P(('clients', 'shard'))
- client_params: bfloat16 [32, 3584], replicated
- client_variate: bfloat16 [32, 3584], replicated
The draws below stay inside these ranges and needn't reach their ends.
Inputs may be any that keep to these rules, and one draw needn't show every extreme that they name: `taking_part`: at least one client takes part.
All inputs are finite; a program needn't handle non-finite values.
Results may differ from the reference program's by a relative error of at most 0.001.
Values may be sent and summed in bfloat16 or wider, within the bound.
A program may use at most 64 MiB of HBM per device.

```python
import jax
import jax.numpy as jnp

D = 3584
CLIENTS = 64
ROWS = 32


def draw_taking_part(key, part):
    random_bits = jax.random.randint(jax.random.fold_in(key, 11), (CLIENTS,), 0, 2)
    picked = jax.random.randint(jax.random.fold_in(key, 12), (), 0, CLIENTS)
    return jnp.where(jnp.arange(CLIENTS) == picked, 1, random_bits).astype(jnp.int32)


def draw_counts(key, part):
    base_count = jax.random.randint(jax.random.fold_in(key, 21), (CLIENTS,), 32, 97)
    return (base_count + 192 * jnp.arange(CLIENTS) // CLIENTS).astype(jnp.int32)


def spiked(values, key, source, target, blocks, factor):
    def block_of(axis_at):
        return (jnp.arange(values.shape[axis_at]) // (values.shape[axis_at] // blocks)).reshape((-1,) + (1,) * (values.ndim - 1 - axis_at))

    one_side = jax.random.permutation(key, blocks)[block_of(target)]
    other_side = (block_of(target) + blocks // 2) % blocks
    return jnp.where((block_of(source) == one_side) | (block_of(source) == other_side), factor * values, values)


def level_of(key, shape, split, low, top_value):
    def one(axis_at, shards_of):
        heights = jax.random.uniform(jax.random.fold_in(jax.random.fold_in(key, 6), axis_at), (shards_of,), jnp.float32, low / len(split), top_value / len(split))
        return jnp.repeat(jnp.exp(heights), shape[axis_at] // shards_of).reshape((-1,) + (1,) * (len(shape) - axis_at - 1))

    loudness = one(*split[0])
    for cut in split[1:]:
        loudness = loudness * one(*cut)
    return loudness


def centred(stream_key, shape, scale, reach, shards=(), held_as=jnp.bfloat16):
    entries = scale * jax.random.normal(stream_key, shape, jnp.float32)
    if shards:
        entries = entries * level_of(stream_key, shape, shards, -0.22, 0.18)
    return jnp.clip(entries, -reach, reach).astype(held_as)


def bell_draw_with(key, shape, scale, limit, shards, heavy, held_as=jnp.bfloat16):
    array = scale * jax.random.normal(key, shape, jnp.float32)
    if shards:
        array = array * level_of(key, shape, shards, -0.22, 0.18)
    return jnp.clip(spiked(array, jax.random.fold_in(key, 3), *heavy), -limit, limit).astype(held_as)


def setup_inputs(seed: int = 0) -> dict:
    keys = jax.random.split(jax.random.key(seed), 7)
    return {
        "client_deltas": bell_draw_with(keys[0], (CLIENTS, ROWS, D), 1.0, 6.0, ((0, 32),), (0, 1, 32, 2.75)),
        "variate_deltas": centred(keys[1], (CLIENTS, ROWS, D), 1.0, 6.0, ((0, 32),)),
        "params": centred(keys[2], (ROWS, D), 0.1, 1.5, ((0, 32),), jnp.float32),
        "variate": centred(keys[3], (ROWS, D), 0.1, 1.5, ((0, 32),), jnp.float32),
        "taking_part": draw_taking_part(jax.random.fold_in(keys[6], 71), 0),
        "counts": draw_counts(jax.random.fold_in(keys[6], 71), 0),
    }


def reference(client_deltas, variate_deltas, params, variate, taking_part, counts):
    weight = taking_part * counts
    upper_part = (weight // 16) * 16
    lower_part = weight - upper_part
    weight_table = jnp.stack([upper_part, lower_part]).astype(jnp.bfloat16)
    weight_total = jnp.sum(weight).astype(jnp.float32)
    moved_sum = jnp.dot(weight_table, client_deltas.reshape(CLIENTS, -1), preferred_element_type=jnp.float32)
    summed = (moved_sum[0] + moved_sum[1]).reshape(ROWS, D)
    chosen = taking_part.astype(jnp.bfloat16)[None, :]
    shifted = jnp.dot(chosen, variate_deltas.reshape(CLIENTS, -1), preferred_element_type=jnp.float32).reshape(ROWS, D)
    new_params = params + summed / weight_total
    new_variate = variate + shifted / jnp.float32(CLIENTS)
    return new_params, new_variate, new_params.astype(jnp.bfloat16), new_variate.astype(jnp.bfloat16)
```

```python
import functools
import math

import jax
import jax.numpy as jnp
from jax import lax
from jax.experimental import pallas as pl
from jax.experimental.pallas import tpu as pltpu
from jax.sharding import PartitionSpec as P

MESH = pl.DeviceIdType.MESH
LANES = 128
CHUNKS = 2


def split_blocks(blocks, parts):
    parts = min(parts, blocks)
    sizes = [blocks // parts + (1 if i < blocks % parts else 0) for i in range(parts)]
    out, at = [], 0
    for size in sizes:
        out.append((at * LANES, size * LANES))
        at += size
    return out


def kernel(
    cfg,
    cd_ref, vd_ref, p_ref, v_ref, tp_ref, ct_ref,
    np_ref, nv_ref, cp_ref, cv_ref,
    mine, theirs, w_send, w_recv, tot_a, tot_b, tot_c, tot_ra, tot_rb,
    prow, send1, recv1, send2, recv2, fin, land, tp_s, ct_s,
    in_sem, d2d_s, d2d_r, w1s, w1r, w2s, w2r, ps, pr, s1s, s1r, s2s, s2r,
    ags, agr, fws, fwr, os, osr, out_sem,
):
    Q, S, C, R, CB, chunks, clients_total = cfg
    local = cd_ref.shape[0]
    cli = lax.axis_index("clients")
    s = lax.axis_index("shard")
    core = lax.rem(cli, 2)
    q = lax.div(cli, 2)
    other = 1 - core
    B = 2 * C
    sr, sc = lax.div(s, C), lax.rem(s, C)

    def dev(qq, cc, ss):
        return (qq * 2 + cc, ss)

    def rcopy(src, dst, ssem, rsem, device):
        return pltpu.make_async_remote_copy(
            src_ref=src, dst_ref=dst, send_sem=ssem, recv_sem=rsem,
            device_id=device, device_id_type=MESH,
        )

    loads = [
        pltpu.make_async_copy(cd_ref, mine.at[0], in_sem.at[0]),
        pltpu.make_async_copy(vd_ref, mine.at[1], in_sem.at[1]),
        pltpu.make_async_copy(tp_ref, tp_s, in_sem.at[2]),
        pltpu.make_async_copy(ct_ref, ct_s, in_sem.at[3]),
    ]
    for load in loads:
        load.start()

    barrier = pltpu.get_barrier_semaphore()
    for t in range(1, Q * S):
        dq, ds = t // S, t % S
        pl.semaphore_signal(
            barrier, inc=1,
            device_id=dev(lax.rem(q + dq, Q), core, lax.rem(s + ds, S)), device_id_type=MESH,
        )
    for ds in range(S):
        pl.semaphore_signal(
            barrier, inc=1, device_id=dev(q, other, lax.rem(s + ds, S)), device_id_type=MESH
        )

    loads[2].wait()
    loads[3].wait()
    own_w = []
    for i in range(local):
        took = tp_s[i]
        weighed = took * ct_s[i]
        here = jnp.where(core == 0, weighed, took).astype(jnp.float32)
        there = jnp.where(core == 0, took, weighed).astype(jnp.float32)
        own_w.append(here)
        w_send[i] = jnp.full((8, LANES), there, jnp.float32)
    loads[0].wait()
    loads[1].wait()

    pl.semaphore_wait(barrier, Q * S - 1 + S)

    partner = dev(q, other, s)
    w_copy = rcopy(w_send, w_recv, d2d_s.at[0], d2d_r.at[0], partner)
    w_copy.start()
    raw_copy = rcopy(mine.at[other], theirs, d2d_s.at[1], d2d_r.at[1], partner)
    raw_copy.start()

    jj = core * S + s
    j_block, j_in = lax.div(jj, B), lax.rem(jj, B)
    for a, src in enumerate((p_ref, v_ref)):
        for c in range(C):
            to_s = j_block * C + c
            me = jnp.logical_and(core == a, s == to_s)
            piece = src.at[:, pl.ds(c * CB, CB)]

            @pl.when(me)
            def _():
                pltpu.make_async_copy(piece, prow.at[j_in], pr.at[j_in]).start()

            @pl.when(jnp.logical_not(me))
            def _():
                rcopy(piece, prow.at[j_in], ps.at[a, c], pr.at[j_in], dev(q, a, to_s)).start()

    w_copy.wait_recv()
    chip_weight = w_recv[0]
    for i in range(1, local):
        chip_weight = chip_weight + w_recv[i]
    for i in range(local):
        chip_weight = chip_weight + own_w[i]
    tot_a[...] = chip_weight

    raw_copy.wait_recv()
    their_w = [w_recv[i][0:1, 0:1] for i in range(local)]

    def plane_copy(k, d):
        off, width = chunks[k]
        to_q = lax.rem(q + d, Q)
        return rcopy(
            send1.at[to_q, :, pl.ds(C * off, C * width)],
            recv1.at[d - 1, :, pl.ds(C * off, C * width)],
            s1s.at[k, d - 1], s1r.at[k, d - 1], dev(to_q, core, s),
        )

    def tot1_copy(d):
        return rcopy(
            tot_a, tot_ra.at[d - 1], w1s.at[d - 1], w1r.at[d - 1],
            dev(lax.rem(q + d, Q), core, s),
        )

    def tot2_copy(e):
        return rcopy(
            tot_b, tot_rb.at[e - 1], w2s.at[e - 1], w2r.at[e - 1],
            dev(q, core, lax.rem(s + e, S)),
        )

    for k, (off, width) in enumerate(chunks):
        for c in range(C):
            cols = slice(c * CB + off, c * CB + off + width)
            acc = None
            for i in range(local):
                term = mine[core, i, :, cols].astype(jnp.float32) * own_w[i]
                acc = term if acc is None else acc + term
                acc = acc + theirs[i, :, cols].astype(jnp.float32) * their_w[i]
            at = C * off + c * width
            send1[:, :, at:at + width] = acc.reshape(Q, 2 * S, width)
        if k == 0:
            for d in range(1, Q):
                tot1_copy(d).start()
        for d in range(1, Q):
            plane_copy(k, d).start()

    def shard_copy(k, e):
        off, width = chunks[k]
        to_s = lax.rem(s + e, S)
        to_r, to_c = lax.div(to_s, C), lax.rem(to_s, C)
        return rcopy(
            send2.at[to_r, :, pl.ds(pl.multiple_of(C * off + to_c * width, LANES), width)],
            recv2.at[e - 1, :, pl.ds(off, width)],
            s2s.at[k, e - 1], s2r.at[k, e - 1], dev(q, core, to_s),
        )

    for k, (off, width) in enumerate(chunks):
        if k == 0:
            plane_weight = tot_a[...]
            for d in range(1, Q):
                tot1_copy(d).wait_recv()
                plane_weight = plane_weight + tot_ra[d - 1]
            tot_b[...] = plane_weight
        for d in range(1, Q):
            plane_copy(k, d).wait_recv()
        cols = slice(C * off, C * (off + width))
        acc = send1[q, :, cols]
        for d in range(1, Q):
            acc = acc + recv1[d - 1, :, cols]
        send2[:, :, cols] = acc.reshape(R, B, C * width)
        if k == 0:
            for e in range(1, S):
                tot2_copy(e).start()
        for e in range(1, S):
            shard_copy(k, e).start()

    block = q * R + sr

    def piece_cols(c, k):
        off, width = chunks[k]
        return pl.ds(pl.multiple_of(c * CB + off, LANES), width)

    def gather_copy(k, t):
        dq, ds = lax.div(t, S), lax.rem(t, S)
        here = land.at[core, block, :, piece_cols(sc, k)]
        return rcopy(
            here, here, ags.at[k, t], agr.at[k, t],
            dev(lax.rem(q + dq, Q), core, lax.rem(s + ds, S)),
        )

    def source_ref(k, t, a):
        dq, ds = lax.div(t, S), lax.rem(t, S)
        from_q, from_s = lax.rem(q + Q - dq, Q), lax.rem(s + S - ds, S)
        return land.at[
            a, from_q * R + lax.div(from_s, C), :, piece_cols(lax.rem(from_s, C), k)
        ]

    def forward_copy(k, t):
        ref = source_ref(k, t, core)
        return rcopy(ref, ref, fws.at[k, t], fwr.at[k, t], partner)

    def forward_recv(k, t):
        ref = source_ref(k, t, other)
        return rcopy(ref, ref, fws.at[k, t], fwr.at[k, t], partner)

    def row_targets(k):
        off, width = chunks[k]
        for j in range(B):
            row = sr * B + j
            to_core, to_s = lax.div(row, S), lax.rem(row, S)
            me = jnp.logical_and(to_core == core, to_s == s)
            yield j, me, dev(q, to_core, to_s), fin.at[j, :, pl.ds(off, width)]

    for k, (off, width) in enumerate(chunks):
        if k == 0:
            weight_total = tot_b[...]
            for e in range(1, S):
                tot2_copy(e).wait_recv()
                weight_total = weight_total + tot_rb[e - 1]
            tot_c[...] = jnp.where(core == 0, weight_total, jnp.float32(clients_total))
            for j in range(B):
                pltpu.make_async_copy(
                    p_ref.at[:, pl.ds(0, CB)], prow.at[j], pr.at[j]
                ).wait()
        for e in range(1, S):
            shard_copy(k, e).wait_recv()
        acc = send2[sr, :, pl.ds(pl.multiple_of(C * off + sc * width, LANES), width)]
        for e in range(1, S):
            acc = acc + recv2[e - 1, :, off:off + width]
        base = jnp.concatenate([prow[j, :, off:off + width] for j in range(B)], axis=0)
        new = base + acc / tot_c[0:1, 0:1]
        land[core, block, :, piece_cols(sc, k)] = new.astype(jnp.bfloat16)
        for j in range(B):
            fin[j, :, off:off + width] = new[j:j + 1, :]

        @pl.loop(1, Q * S)
        def _(t):
            gather_copy(k, t).start()

        forward_copy(k, 0).start()
        for a, out in enumerate((np_ref, nv_ref)):
            @pl.when(core == a)
            def _():
                for j, me, device, src in row_targets(k):
                    dst = out.at[:, piece_cols(sc, k)]

                    @pl.when(me)
                    def _():
                        pltpu.make_async_copy(src, dst, osr.at[a, sc, k]).start()

                    @pl.when(jnp.logical_not(me))
                    def _():
                        rcopy(src, dst, os.at[j, k], osr.at[a, sc, k], device).start()

    for k in range(len(chunks)):
        @pl.loop(1, Q * S)
        def _(t):
            gather_copy(k, t).wait_recv()
            forward_copy(k, t).start()

    for k in range(len(chunks)):
        @pl.loop(0, Q * S)
        def _(t):
            forward_recv(k, t).wait_recv()

    outs = [
        pltpu.make_async_copy(land.at[0], cp_ref, out_sem.at[0]),
        pltpu.make_async_copy(land.at[1], cv_ref, out_sem.at[1]),
    ]
    for out in outs:
        out.start()

    w_copy.wait_send()
    raw_copy.wait_send()
    for a, src in enumerate((p_ref, v_ref)):
        for c in range(C):
            to_s = j_block * C + c
            me = jnp.logical_and(core == a, s == to_s)

            @pl.when(jnp.logical_not(me))
            def _():
                rcopy(
                    src.at[:, pl.ds(c * CB, CB)], prow.at[j_in], ps.at[a, c], pr.at[j_in],
                    dev(q, a, to_s),
                ).wait_send()
    for d in range(1, Q):
        tot1_copy(d).wait_send()
    for e in range(1, S):
        tot2_copy(e).wait_send()
    for k, (off, width) in enumerate(chunks):
        for d in range(1, Q):
            plane_copy(k, d).wait_send()
        for e in range(1, S):
            shard_copy(k, e).wait_send()

        @pl.loop(1, Q * S)
        def _(t):
            gather_copy(k, t).wait_send()

        @pl.loop(0, Q * S)
        def _(t):
            forward_copy(k, t).wait_send()

        for j, me, device, src in row_targets(k):
            @pl.when(jnp.logical_not(me))
            def _():
                rcopy(
                    src, np_ref.at[:, piece_cols(sc, k)], os.at[j, k], osr.at[0, sc, k], device
                ).wait_send()
        for a, out in enumerate((np_ref, nv_ref)):
            for c in range(C):
                pltpu.make_async_copy(
                    fin.at[0, :, pl.ds(off, width)], out.at[:, piece_cols(c, k)],
                    osr.at[a, c, k],
                ).wait()
    for out in outs:
        out.wait()


def body(sizes, client_deltas, variate_deltas, params, variate, taking_part, counts):
    n_clients, S = sizes
    Q = n_clients // 2
    local, rows, D = client_deltas.shape
    C = math.gcd(S, D // LANES)
    R = S // C
    B = 2 * C
    CB = D // C
    chunks = split_blocks(CB // LANES, CHUNKS)
    K = len(chunks)
    cfg = (Q, S, C, R, CB, chunks, local * n_clients * S)
    f32, bf16 = jnp.float32, jnp.bfloat16
    DMA = pltpu.SemaphoreType.DMA
    any_spec = pl.BlockSpec(memory_space=pl.ANY)
    blocks = rows // B
    new_params, new_variate, cp, cv = pl.pallas_call(
        functools.partial(kernel, cfg),
        out_shape=(
            jax.ShapeDtypeStruct((1, D), f32),
            jax.ShapeDtypeStruct((1, D), f32),
            jax.ShapeDtypeStruct((blocks, B, D), bf16),
            jax.ShapeDtypeStruct((blocks, B, D), bf16),
        ),
        in_specs=[any_spec] * 6,
        out_specs=(any_spec,) * 4,
        scratch_shapes=[
            pltpu.VMEM((2, local, rows, D), bf16),
            pltpu.VMEM((local, rows, D), bf16),
            pltpu.VMEM((local, 8, LANES), f32),
            pltpu.VMEM((local, 8, LANES), f32),
            pltpu.VMEM((8, LANES), f32),
            pltpu.VMEM((8, LANES), f32),
            pltpu.VMEM((8, LANES), f32),
            pltpu.VMEM((Q - 1, 8, LANES), f32),
            pltpu.VMEM((S - 1, 8, LANES), f32),
            pltpu.VMEM((B, 1, CB), f32),
            pltpu.VMEM((Q, 2 * S, D), f32),
            pltpu.VMEM((Q - 1, 2 * S, D), f32),
            pltpu.VMEM((R, B, D), f32),
            pltpu.VMEM((S - 1, B, CB), f32),
            pltpu.VMEM((B, 1, CB), f32),
            pltpu.VMEM((2, blocks, B, D), bf16),
            pltpu.SMEM((local,), jnp.int32),
            pltpu.SMEM((local,), jnp.int32),
            DMA((4,)), DMA((2,)), DMA((2,)),
            DMA((Q - 1,)), DMA((Q - 1,)), DMA((S - 1,)), DMA((S - 1,)),
            DMA((2, C)), DMA((B,)),
            DMA((K, Q - 1)), DMA((K, Q - 1)), DMA((K, S - 1)), DMA((K, S - 1)),
            DMA((K, Q * S)), DMA((K, Q * S)), DMA((K, Q * S)), DMA((K, Q * S)),
            DMA((B, K)), DMA((2, C, K)), DMA((2,)),
        ],
        compiler_params=pltpu.CompilerParams(collective_id=0, has_side_effects=True),
    )(client_deltas, variate_deltas, params, variate, taking_part, counts)
    return new_params, new_variate, cp.reshape(rows, D), cv.reshape(rows, D)


def solution(mesh):
    both = ("clients", "shard")
    in_specs = (
        P(both, None, None),
        P(both, None, None),
        P(both, None),
        P(both, None),
        P(both),
        P(both),
    )
    out_specs = (P(both, None), P(both, None), P(), P())
    sizes = (mesh.shape["clients"], mesh.shape["shard"])
    return jax.shard_map(
        functools.partial(body, sizes),
        mesh=mesh, in_specs=in_specs, out_specs=out_specs, check_vma=False,
    )
```

```python
import functools
import math

import jax
import jax.numpy as jnp
from jax import lax
from jax.experimental import pallas as pl
from jax.experimental.pallas import tpu as pltpu
from jax.sharding import PartitionSpec as P

MESH = pl.DeviceIdType.MESH
LANES = 128
CHUNKS = 2
RELAY = False
NEAR = True


def split_blocks(blocks, parts):
    parts = min(parts, blocks)
    sizes = [blocks // parts + (1 if i < blocks % parts else 0) for i in range(parts)]
    out, at = [], 0
    for size in sizes:
        out.append((at * LANES, size * LANES))
        at += size
    return out


def kernel(
    cfg,
    cd_ref, vd_ref, p_ref, v_ref, tp_ref, ct_ref,
    rows, land,
    mine, theirs, w_send, w_recv, tot_a, tot_b, tot_c, tot_ra, tot_rb,
    prow, send1, recv1, send2, recv2, fin, tp_s, ct_s,
    in_sem, d2d_s, d2d_r, w1s, w1r, w2s, w2r, ps, pr, s1s, s1r, s2s, s2r,
    ags, agr, fws, fwr, os, osr,
):
    Q, S, C, R, CB, chunks, clients_total = cfg
    local = cd_ref.shape[0]
    cli = lax.axis_index("clients")
    s = lax.axis_index("shard")
    core = lax.rem(cli, 2)
    q = lax.div(cli, 2)
    other = 1 - core
    B = 2 * C
    sr, sc = lax.div(s, C), lax.rem(s, C)

    def dev(qq, cc, ss):
        return (qq * 2 + cc, ss)

    def rcopy(src, dst, ssem, rsem, device):
        return pltpu.make_async_remote_copy(
            src_ref=src, dst_ref=dst, send_sem=ssem, recv_sem=rsem,
            device_id=device, device_id_type=MESH,
        )

    loads = [
        pltpu.make_async_copy(cd_ref, mine.at[0], in_sem.at[0]),
        pltpu.make_async_copy(vd_ref, mine.at[1], in_sem.at[1]),
        pltpu.make_async_copy(tp_ref, tp_s, in_sem.at[2]),
        pltpu.make_async_copy(ct_ref, ct_s, in_sem.at[3]),
    ]
    for load in loads:
        load.start()

    barrier = pltpu.get_barrier_semaphore()
    greeted = S
    for t in range(1, Q * S):
        dq, ds = t // S, t % S
        if NEAR and dq and ds:
            continue
        greeted += 1
        pl.semaphore_signal(
            barrier, inc=1,
            device_id=dev(lax.rem(q + dq, Q), core, lax.rem(s + ds, S)), device_id_type=MESH,
        )
    for ds in range(S):
        pl.semaphore_signal(
            barrier, inc=1, device_id=dev(q, other, lax.rem(s + ds, S)), device_id_type=MESH
        )

    loads[2].wait()
    loads[3].wait()
    own_w = []
    for i in range(local):
        took = tp_s[i]
        weighed = took * ct_s[i]
        here = jnp.where(core == 0, weighed, took).astype(jnp.float32)
        there = jnp.where(core == 0, took, weighed).astype(jnp.float32)
        own_w.append(here)
        w_send[i] = jnp.full((8, LANES), there, jnp.float32)
    loads[0].wait()
    loads[1].wait()

    pl.semaphore_wait(barrier, greeted)

    partner = dev(q, other, s)
    w_copy = rcopy(w_send, w_recv, d2d_s.at[0], d2d_r.at[0], partner)
    w_copy.start()
    raw_copy = rcopy(mine.at[other], theirs, d2d_s.at[1], d2d_r.at[1], partner)
    raw_copy.start()

    jj = core * S + s
    j_block, j_in = lax.div(jj, B), lax.rem(jj, B)
    for a, src in enumerate((p_ref, v_ref)):
        for c in range(C):
            to_s = j_block * C + c
            me = jnp.logical_and(core == a, s == to_s)
            piece = src.at[:, pl.ds(c * CB, CB)]

            @pl.when(me)
            def _():
                pltpu.make_async_copy(piece, prow.at[j_in], pr.at[j_in]).start()

            @pl.when(jnp.logical_not(me))
            def _():
                rcopy(piece, prow.at[j_in], ps.at[a, c], pr.at[j_in], dev(q, a, to_s)).start()

    w_copy.wait_recv()
    chip_weight = w_recv[0]
    for i in range(1, local):
        chip_weight = chip_weight + w_recv[i]
    for i in range(local):
        chip_weight = chip_weight + own_w[i]
    tot_a[...] = chip_weight

    raw_copy.wait_recv()
    their_w = [w_recv[i][0:1, 0:1] for i in range(local)]

    def plane_copy(k, d):
        off, width = chunks[k]
        to_q = lax.rem(q + d, Q)
        return rcopy(
            send1.at[to_q, :, pl.ds(C * off, C * width)],
            recv1.at[d - 1, :, pl.ds(C * off, C * width)],
            s1s.at[k, d - 1], s1r.at[k, d - 1], dev(to_q, core, s),
        )

    def tot1_copy(d):
        return rcopy(
            tot_a, tot_ra.at[d - 1], w1s.at[d - 1], w1r.at[d - 1],
            dev(lax.rem(q + d, Q), core, s),
        )

    def tot2_copy(e):
        return rcopy(
            tot_b, tot_rb.at[e - 1], w2s.at[e - 1], w2r.at[e - 1],
            dev(q, core, lax.rem(s + e, S)),
        )

    for k, (off, width) in enumerate(chunks):
        for c in range(C):
            cols = slice(c * CB + off, c * CB + off + width)
            acc = None
            for i in range(local):
                term = mine[core, i, :, cols].astype(jnp.float32) * own_w[i]
                acc = term if acc is None else acc + term
                acc = acc + theirs[i, :, cols].astype(jnp.float32) * their_w[i]
            at = C * off + c * width
            send1[:, :, at:at + width] = acc.reshape(Q, 2 * S, width)
        if k == 0:
            for d in range(1, Q):
                tot1_copy(d).start()
        for d in range(1, Q):
            plane_copy(k, d).start()

    def shard_copy(k, e):
        off, width = chunks[k]
        to_s = lax.rem(s + e, S)
        to_r, to_c = lax.div(to_s, C), lax.rem(to_s, C)
        return rcopy(
            send2.at[to_r, :, pl.ds(pl.multiple_of(C * off + to_c * width, LANES), width)],
            recv2.at[e - 1, :, pl.ds(off, width)],
            s2s.at[k, e - 1], s2r.at[k, e - 1], dev(q, core, to_s),
        )

    for k, (off, width) in enumerate(chunks):
        if k == 0:
            plane_weight = tot_a[...]
            for d in range(1, Q):
                tot1_copy(d).wait_recv()
                plane_weight = plane_weight + tot_ra[d - 1]
            tot_b[...] = plane_weight
        for d in range(1, Q):
            plane_copy(k, d).wait_recv()
        cols = slice(C * off, C * (off + width))
        acc = send1[q, :, cols]
        for d in range(1, Q):
            acc = acc + recv1[d - 1, :, cols]
        send2[:, :, cols] = acc.reshape(R, B, C * width)
        if k == 0:
            for e in range(1, S):
                tot2_copy(e).start()
        for e in range(1, S):
            shard_copy(k, e).start()

    block = q * R + sr

    def piece_cols(c, k):
        off, width = chunks[k]
        return pl.ds(pl.multiple_of(c * CB + off, LANES), width)

    def gather_copy(k, t):
        dq, ds = lax.div(t, S), lax.rem(t, S)
        here = land.at[core, block, :, piece_cols(sc, k)]
        return rcopy(
            here, here, ags.at[k, t], agr.at[k, t],
            dev(lax.rem(q + dq, Q), core, lax.rem(s + ds, S)),
        )

    def source_ref(k, t, a):
        dq, ds = lax.div(t, S), lax.rem(t, S)
        from_q, from_s = lax.rem(q + Q - dq, Q), lax.rem(s + S - ds, S)
        return land.at[
            a, from_q * R + lax.div(from_s, C), :, piece_cols(lax.rem(from_s, C), k)
        ]

    def relay_copy(k, d, e):
        ref = source_ref(k, jnp.int32(e), core)
        return rcopy(
            ref, ref, ags.at[k, d * S + e], agr.at[k, d * S + e], dev(lax.rem(q + d, Q), core, s)
        )

    def row_copy(k, j, src, device):
        dst = rows.at[core, :, piece_cols(sc, k)]
        return rcopy(src, dst, os.at[j, k], osr.at[core, sc, k], device)

    def forward_copy(k, t):
        ref = source_ref(k, t, core)
        return rcopy(ref, ref, fws.at[k, t], fwr.at[k, t], partner)

    def forward_recv(k, t):
        ref = source_ref(k, t, other)
        return rcopy(ref, ref, fws.at[k, t], fwr.at[k, t], partner)

    def row_targets(k):
        off, width = chunks[k]
        for j in range(B):
            row = sr * B + j
            to_core, to_s = lax.div(row, S), lax.rem(row, S)
            me = jnp.logical_and(to_core == core, to_s == s)
            yield j, me, dev(q, to_core, to_s), fin.at[j, :, pl.ds(off, width)]

    for k, (off, width) in enumerate(chunks):
        if k == 0:
            weight_total = tot_b[...]
            for e in range(1, S):
                tot2_copy(e).wait_recv()
                weight_total = weight_total + tot_rb[e - 1]
            tot_c[...] = jnp.where(core == 0, weight_total, jnp.float32(clients_total))
            for j in range(B):
                pltpu.make_async_copy(
                    p_ref.at[:, pl.ds(0, CB)], prow.at[j], pr.at[j]
                ).wait()
        for e in range(1, S):
            shard_copy(k, e).wait_recv()
        acc = send2[sr, :, pl.ds(pl.multiple_of(C * off + sc * width, LANES), width)]
        for e in range(1, S):
            acc = acc + recv2[e - 1, :, off:off + width]
        base = jnp.concatenate([prow[j, :, off:off + width] for j in range(B)], axis=0)
        new = base + acc / tot_c[0:1, 0:1]
        land[core, block, :, piece_cols(sc, k)] = new.astype(jnp.bfloat16)
        for j in range(B):
            fin[j, :, off:off + width] = new[j:j + 1, :]

        if RELAY:
            for e in range(1, S):
                gather_copy(k, e).start()
            for d in range(1, Q):
                relay_copy(k, d, 0).start()
        else:
            @pl.loop(1, Q * S)
            def _(t):
                gather_copy(k, t).start()

        forward_copy(k, 0).start()
        for j, me, device, src in row_targets(k):
            @pl.when(jnp.logical_not(me))
            def _():
                row_copy(k, j, src, device).start()

        @pl.when(j_block == sr)
        def _():
            rows[core, :, piece_cols(sc, k)] = fin[j_in, :, off:off + width]

    if RELAY:
        for k in range(len(chunks)):
            for e in range(1, S):
                gather_copy(k, e).wait_recv()
                for d in range(1, Q):
                    relay_copy(k, d, e).start()
                forward_copy(k, e).start()
    for k in range(len(chunks)):
        @pl.loop(S if RELAY else 1, Q * S)
        def _(t):
            gather_copy(k, t).wait_recv()
            forward_copy(k, t).start()

    for k in range(len(chunks)):
        @pl.loop(0, Q * S)
        def _(t):
            forward_recv(k, t).wait_recv()

    w_copy.wait_send()
    raw_copy.wait_send()
    for a, src in enumerate((p_ref, v_ref)):
        for c in range(C):
            to_s = j_block * C + c
            me = jnp.logical_and(core == a, s == to_s)

            @pl.when(jnp.logical_not(me))
            def _():
                rcopy(
                    src.at[:, pl.ds(c * CB, CB)], prow.at[j_in], ps.at[a, c], pr.at[j_in],
                    dev(q, a, to_s),
                ).wait_send()
    for d in range(1, Q):
        tot1_copy(d).wait_send()
    for e in range(1, S):
        tot2_copy(e).wait_send()
    for k, (off, width) in enumerate(chunks):
        for d in range(1, Q):
            plane_copy(k, d).wait_send()
        for e in range(1, S):
            shard_copy(k, e).wait_send()

        if RELAY:
            for e in range(S):
                if e:
                    gather_copy(k, e).wait_send()
                for d in range(1, Q):
                    relay_copy(k, d, e).wait_send()
        else:
            @pl.loop(1, Q * S)
            def _(t):
                gather_copy(k, t).wait_send()

        @pl.loop(0, Q * S)
        def _(t):
            forward_copy(k, t).wait_send()

        for j, me, device, src in row_targets(k):
            @pl.when(jnp.logical_not(me))
            def _():
                row_copy(k, j, src, device).wait_send()
        for a in range(2):
            for c in range(C):
                me = jnp.logical_and(core == a, s == j_block * C + c)

                @pl.when(jnp.logical_not(me))
                def _():
                    rcopy(
                        fin.at[0, :, pl.ds(off, width)], rows.at[a, :, piece_cols(c, k)],
                        os.at[0, k], osr.at[a, c, k], partner,
                    ).wait_recv()


def store_kernel(rows, land, np_ref, nv_ref, cp_ref, cv_ref, sem):
    copies = [
        pltpu.make_async_copy(land.at[0], cp_ref, sem.at[0]),
        pltpu.make_async_copy(land.at[1], cv_ref, sem.at[1]),
        pltpu.make_async_copy(rows.at[0], np_ref, sem.at[2]),
        pltpu.make_async_copy(rows.at[1], nv_ref, sem.at[3]),
    ]
    for copy in copies:
        copy.start()
    for copy in copies:
        copy.wait()


def body(sizes, client_deltas, variate_deltas, params, variate, taking_part, counts):
    n_clients, S = sizes
    Q = n_clients // 2
    local, rows, D = client_deltas.shape
    C = math.gcd(S, D // LANES)
    R = S // C
    B = 2 * C
    CB = D // C
    chunks = split_blocks(CB // LANES, CHUNKS)
    K = len(chunks)
    cfg = (Q, S, C, R, CB, chunks, local * n_clients * S)
    f32, bf16 = jnp.float32, jnp.bfloat16
    DMA = pltpu.SemaphoreType.DMA
    any_spec = pl.BlockSpec(memory_space=pl.ANY)
    blocks = rows // B
    vmem_spec = pl.BlockSpec(memory_space=pltpu.VMEM)
    new_rows, land = pl.pallas_call(
        functools.partial(kernel, cfg),
        out_shape=(pltpu.VMEM((2, 1, D), f32), pltpu.VMEM((2, blocks, B, D), bf16)),
        in_specs=[any_spec] * 6,
        out_specs=(vmem_spec,) * 2,
        scratch_shapes=[
            pltpu.VMEM((2, local, rows, D), bf16),
            pltpu.VMEM((local, rows, D), bf16),
            pltpu.VMEM((local, 8, LANES), f32),
            pltpu.VMEM((local, 8, LANES), f32),
            pltpu.VMEM((8, LANES), f32),
            pltpu.VMEM((8, LANES), f32),
            pltpu.VMEM((8, LANES), f32),
            pltpu.VMEM((Q - 1, 8, LANES), f32),
            pltpu.VMEM((S - 1, 8, LANES), f32),
            pltpu.VMEM((B, 1, CB), f32),
            pltpu.VMEM((Q, 2 * S, D), f32),
            pltpu.VMEM((Q - 1, 2 * S, D), f32),
            pltpu.VMEM((R, B, D), f32),
            pltpu.VMEM((S - 1, B, CB), f32),
            pltpu.VMEM((B, 1, CB), f32),
            pltpu.SMEM((local,), jnp.int32),
            pltpu.SMEM((local,), jnp.int32),
            DMA((4,)), DMA((2,)), DMA((2,)),
            DMA((Q - 1,)), DMA((Q - 1,)), DMA((S - 1,)), DMA((S - 1,)),
            DMA((2, C)), DMA((B,)),
            DMA((K, Q - 1)), DMA((K, Q - 1)), DMA((K, S - 1)), DMA((K, S - 1)),
            DMA((K, Q * S)), DMA((K, Q * S)), DMA((K, Q * S)), DMA((K, Q * S)),
            DMA((B, K)), DMA((2, C, K)),
        ],
        compiler_params=pltpu.CompilerParams(collective_id=0, has_side_effects=True),
    )(client_deltas, variate_deltas, params, variate, taking_part, counts)
    new_params, new_variate, cp, cv = pl.pallas_call(
        store_kernel,
        out_shape=(
            jax.ShapeDtypeStruct((1, D), f32),
            jax.ShapeDtypeStruct((1, D), f32),
            jax.ShapeDtypeStruct((blocks, B, D), bf16),
            jax.ShapeDtypeStruct((blocks, B, D), bf16),
        ),
        in_specs=[vmem_spec] * 2,
        out_specs=(any_spec,) * 4,
        scratch_shapes=[DMA((4,))],
    )(new_rows, land)
    return new_params, new_variate, cp.reshape(rows, D), cv.reshape(rows, D)


def solution(mesh):
    both = ("clients", "shard")
    in_specs = (
        P(both, None, None),
        P(both, None, None),
        P(both, None),
        P(both, None),
        P(both),
        P(both),
    )
    out_specs = (P(both, None), P(both, None), P(), P())
    sizes = (mesh.shape["clients"], mesh.shape["shard"])
    return jax.shard_map(
        functools.partial(body, sizes),
        mesh=mesh, in_specs=in_specs, out_specs=out_specs, check_vma=False,
    )
```

```python
import functools
import math

import jax
import jax.numpy as jnp
from jax import lax
from jax.experimental import pallas as pl
from jax.experimental.pallas import tpu as pltpu
from jax.sharding import PartitionSpec as P

MESH = pl.DeviceIdType.MESH
LANES = 128
CHUNKS = 2
RELAY = False
NEAR = True


def split_blocks(blocks, parts):
    parts = min(parts, blocks)
    sizes = [blocks // parts + (1 if i < blocks % parts else 0) for i in range(parts)]
    out, at = [], 0
    for size in sizes:
        out.append((at * LANES, size * LANES))
        at += size
    return out


def kernel(
    cfg,
    cd_ref, vd_ref, p_ref, v_ref, tp_ref, ct_ref,
    rows, land,
    mine, theirs, w_send, w_recv, tot_a, tot_b, tot_c, tot_ra, tot_rb,
    prow, send1, recv1, send2, recv2, fin, tp_s, ct_s,
    in_sem, d2d_s, d2d_r, w1s, w1r, w2s, w2r, ps, pr, s1s, s1r, s2s, s2r,
    ags, agr, fws, fwr, os, osr,
):
    Q, S, C, R, CB, chunks, clients_total = cfg
    local = cd_ref.shape[0]
    cli = lax.axis_index("clients")
    s = lax.axis_index("shard")
    core = lax.rem(cli, 2)
    q = lax.div(cli, 2)
    other = 1 - core
    B = 2 * C
    sr, sc = lax.div(s, C), lax.rem(s, C)

    def dev(qq, cc, ss):
        return (qq * 2 + cc, ss)

    def rcopy(src, dst, ssem, rsem, device):
        return pltpu.make_async_remote_copy(
            src_ref=src, dst_ref=dst, send_sem=ssem, recv_sem=rsem,
            device_id=device, device_id_type=MESH,
        )

    loads = [
        pltpu.make_async_copy(cd_ref, mine.at[0], in_sem.at[0]),
        pltpu.make_async_copy(vd_ref, mine.at[1], in_sem.at[1]),
        pltpu.make_async_copy(tp_ref, tp_s, in_sem.at[2]),
        pltpu.make_async_copy(ct_ref, ct_s, in_sem.at[3]),
    ]
    for load in loads:
        load.start()

    barrier = pltpu.get_barrier_semaphore()
    greeted = S
    for t in range(1, Q * S):
        dq, ds = t // S, t % S
        if NEAR and dq and ds:
            continue
        greeted += 1
        pl.semaphore_signal(
            barrier, inc=1,
            device_id=dev(lax.rem(q + dq, Q), core, lax.rem(s + ds, S)), device_id_type=MESH,
        )
    for ds in range(S):
        pl.semaphore_signal(
            barrier, inc=1, device_id=dev(q, other, lax.rem(s + ds, S)), device_id_type=MESH
        )

    loads[2].wait()
    loads[3].wait()
    own_w = []
    for i in range(local):
        took = tp_s[i]
        weighed = took * ct_s[i]
        here = jnp.where(core == 0, weighed, took).astype(jnp.float32)
        there = jnp.where(core == 0, took, weighed).astype(jnp.float32)
        own_w.append(here)
        w_send[i] = jnp.full((8, LANES), there, jnp.float32)
    loads[0].wait()
    loads[1].wait()

    pl.semaphore_wait(barrier, greeted)

    partner = dev(q, other, s)
    w_copy = rcopy(w_send, w_recv, d2d_s.at[0], d2d_r.at[0], partner)
    w_copy.start()
    raw_copy = rcopy(mine.at[other], theirs, d2d_s.at[1], d2d_r.at[1], partner)
    raw_copy.start()

    jj = core * S + s
    j_block, j_in = lax.div(jj, B), lax.rem(jj, B)
    for a, src in enumerate((p_ref, v_ref)):
        for c in range(C):
            to_s = j_block * C + c
            me = jnp.logical_and(core == a, s == to_s)
            piece = src.at[:, pl.ds(c * CB, CB)]

            @pl.when(me)
            def _():
                pltpu.make_async_copy(piece, prow.at[j_in], pr.at[j_in]).start()

            @pl.when(jnp.logical_not(me))
            def _():
                rcopy(piece, prow.at[j_in], ps.at[a, c], pr.at[j_in], dev(q, a, to_s)).start()

    w_copy.wait_recv()
    chip_weight = w_recv[0]
    for i in range(1, local):
        chip_weight = chip_weight + w_recv[i]
    for i in range(local):
        chip_weight = chip_weight + own_w[i]
    tot_a[...] = chip_weight

    raw_copy.wait_recv()
    their_w = [w_recv[i][0:1, 0:1] for i in range(local)]

    def plane_copy(k, d):
        off, width = chunks[k]
        to_q = lax.rem(q + d, Q)
        return rcopy(
            send1.at[to_q, :, pl.ds(C * off, C * width)],
            recv1.at[d - 1, :, pl.ds(C * off, C * width)],
            s1s.at[k, d - 1], s1r.at[k, d - 1], dev(to_q, core, s),
        )

    def tot1_copy(d):
        return rcopy(
            tot_a, tot_ra.at[d - 1], w1s.at[d - 1], w1r.at[d - 1],
            dev(lax.rem(q + d, Q), core, s),
        )

    def tot2_copy(e):
        return rcopy(
            tot_b, tot_rb.at[e - 1], w2s.at[e - 1], w2r.at[e - 1],
            dev(q, core, lax.rem(s + e, S)),
        )

    for k, (off, width) in enumerate(chunks):
        for c in range(C):
            cols = slice(c * CB + off, c * CB + off + width)
            acc = None
            for i in range(local):
                term = mine[core, i, :, cols].astype(jnp.float32) * own_w[i]
                acc = term if acc is None else acc + term
                acc = acc + theirs[i, :, cols].astype(jnp.float32) * their_w[i]
            at = C * off + c * width
            send1[:, :, at:at + width] = acc.reshape(Q, 2 * S, width)
        if k == 0:
            for d in range(1, Q):
                tot1_copy(d).start()
        for d in range(1, Q):
            plane_copy(k, d).start()

    def shard_copy(k, e):
        off, width = chunks[k]
        to_s = lax.rem(s + e, S)
        to_r, to_c = lax.div(to_s, C), lax.rem(to_s, C)
        return rcopy(
            send2.at[to_r, :, pl.ds(pl.multiple_of(C * off + to_c * width, LANES), width)],
            recv2.at[e - 1, :, pl.ds(off, width)],
            s2s.at[k, e - 1], s2r.at[k, e - 1], dev(q, core, to_s),
        )

    for k, (off, width) in enumerate(chunks):
        if k == 0:
            plane_weight = tot_a[...]
            for d in range(1, Q):
                tot1_copy(d).wait_recv()
                plane_weight = plane_weight + tot_ra[d - 1]
            tot_b[...] = plane_weight
        for d in range(1, Q):
            plane_copy(k, d).wait_recv()
        cols = slice(C * off, C * (off + width))
        acc = send1[q, :, cols]
        for d in range(1, Q):
            acc = acc + recv1[d - 1, :, cols]
        send2[:, :, cols] = acc.reshape(R, B, C * width)
        if k == 0:
            for e in range(1, S):
                tot2_copy(e).start()
        for e in range(1, S):
            shard_copy(k, e).start()

    block = q * R + sr

    def piece_cols(c, k):
        off, width = chunks[k]
        return pl.ds(pl.multiple_of(c * CB + off, LANES), width)

    def gather_copy(k, t):
        dq, ds = lax.div(t, S), lax.rem(t, S)
        here = land.at[core, block, :, piece_cols(sc, k)]
        return rcopy(
            here, here, ags.at[k, t], agr.at[k, t],
            dev(lax.rem(q + dq, Q), core, lax.rem(s + ds, S)),
        )

    def source_ref(k, t, a):
        dq, ds = lax.div(t, S), lax.rem(t, S)
        from_q, from_s = lax.rem(q + Q - dq, Q), lax.rem(s + S - ds, S)
        return land.at[
            a, from_q * R + lax.div(from_s, C), :, piece_cols(lax.rem(from_s, C), k)
        ]

    def relay_copy(k, d, e):
        ref = source_ref(k, jnp.int32(e), core)
        return rcopy(
            ref, ref, ags.at[k, d * S + e], agr.at[k, d * S + e], dev(lax.rem(q + d, Q), core, s)
        )

    def row_copy(k, j, src, device):
        dst = rows.at[core, :, piece_cols(sc, k)]
        return rcopy(src, dst, os.at[j, k], osr.at[core, sc, k], device)

    def forward_copy(k, t):
        ref = source_ref(k, t, core)
        return rcopy(ref, ref, fws.at[k, t], fwr.at[k, t], partner)

    def forward_recv(k, t):
        ref = source_ref(k, t, other)
        return rcopy(ref, ref, fws.at[k, t], fwr.at[k, t], partner)

    def row_targets(k):
        off, width = chunks[k]
        for j in range(B):
            row = sr * B + j
            to_core, to_s = lax.div(row, S), lax.rem(row, S)
            me = jnp.logical_and(to_core == core, to_s == s)
            yield j, me, dev(q, to_core, to_s), fin.at[j, :, pl.ds(off, width)]

    for k, (off, width) in enumerate(chunks):
        if k == 0:
            weight_total = tot_b[...]
            for e in range(1, S):
                tot2_copy(e).wait_recv()
                weight_total = weight_total + tot_rb[e - 1]
            tot_c[...] = jnp.where(core == 0, weight_total, jnp.float32(clients_total))
            for j in range(B):
                pltpu.make_async_copy(
                    p_ref.at[:, pl.ds(0, CB)], prow.at[j], pr.at[j]
                ).wait()
        for e in range(1, S):
            shard_copy(k, e).wait_recv()
        acc = send2[sr, :, pl.ds(pl.multiple_of(C * off + sc * width, LANES), width)]
        for e in range(1, S):
            acc = acc + recv2[e - 1, :, off:off + width]
        base = jnp.concatenate([prow[j, :, off:off + width] for j in range(B)], axis=0)
        new = base + acc / tot_c[0:1, 0:1]
        land[core, block, :, piece_cols(sc, k)] = new.astype(jnp.bfloat16)
        for j in range(B):
            fin[j, :, off:off + width] = new[j:j + 1, :]

        if RELAY:
            for e in range(1, S):
                gather_copy(k, e).start()
            for d in range(1, Q):
                relay_copy(k, d, 0).start()
        else:
            @pl.loop(1, Q * S)
            def _(t):
                gather_copy(k, t).start()

        forward_copy(k, 0).start()
        for j, me, device, src in row_targets(k):
            @pl.when(jnp.logical_not(me))
            def _():
                row_copy(k, j, src, device).start()

        @pl.when(j_block == sr)
        def _():
            rows[core, :, piece_cols(sc, k)] = fin[j_in, :, off:off + width]

    if RELAY:
        for k in range(len(chunks)):
            for e in range(1, S):
                gather_copy(k, e).wait_recv()
                for d in range(1, Q):
                    relay_copy(k, d, e).start()
                forward_copy(k, e).start()
    for k in range(len(chunks)):
        @pl.loop(S if RELAY else 1, Q * S)
        def _(t):
            gather_copy(k, t).wait_recv()
            forward_copy(k, t).start()

    for k in range(len(chunks)):
        @pl.loop(0, Q * S)
        def _(t):
            forward_recv(k, t).wait_recv()

    w_copy.wait_send()
    raw_copy.wait_send()
    for a, src in enumerate((p_ref, v_ref)):
        for c in range(C):
            to_s = j_block * C + c
            me = jnp.logical_and(core == a, s == to_s)

            @pl.when(jnp.logical_not(me))
            def _():
                rcopy(
                    src.at[:, pl.ds(c * CB, CB)], prow.at[j_in], ps.at[a, c], pr.at[j_in],
                    dev(q, a, to_s),
                ).wait_send()
    for d in range(1, Q):
        tot1_copy(d).wait_send()
    for e in range(1, S):
        tot2_copy(e).wait_send()
    for k, (off, width) in enumerate(chunks):
        for d in range(1, Q):
            plane_copy(k, d).wait_send()
        for e in range(1, S):
            shard_copy(k, e).wait_send()

        if RELAY:
            for e in range(S):
                if e:
                    gather_copy(k, e).wait_send()
                for d in range(1, Q):
                    relay_copy(k, d, e).wait_send()
        else:
            @pl.loop(1, Q * S)
            def _(t):
                gather_copy(k, t).wait_send()

        @pl.loop(0, Q * S)
        def _(t):
            forward_copy(k, t).wait_send()

        for j, me, device, src in row_targets(k):
            @pl.when(jnp.logical_not(me))
            def _():
                row_copy(k, j, src, device).wait_send()
        for a in range(2):
            for c in range(C):
                me = jnp.logical_and(core == a, s == j_block * C + c)

                @pl.when(jnp.logical_not(me))
                def _():
                    rcopy(
                        fin.at[0, :, pl.ds(off, width)], rows.at[a, :, piece_cols(c, k)],
                        os.at[0, k], osr.at[a, c, k], partner,
                    ).wait_recv()


def store_kernel(rows, land, np_ref, nv_ref, cp_ref, cv_ref, sem):
    copies = [
        pltpu.make_async_copy(land.at[0], cp_ref, sem.at[0]),
        pltpu.make_async_copy(land.at[1], cv_ref, sem.at[1]),
        pltpu.make_async_copy(rows.at[0], np_ref, sem.at[2]),
        pltpu.make_async_copy(rows.at[1], nv_ref, sem.at[3]),
    ]
    for copy in copies:
        copy.start()
    for copy in copies:
        copy.wait()


def body(sizes, client_deltas, variate_deltas, params, variate, taking_part, counts):
    n_clients, S = sizes
    Q = n_clients // 2
    local, rows, D = client_deltas.shape
    C = math.gcd(S, D // LANES)
    R = S // C
    B = 2 * C
    CB = D // C
    chunks = split_blocks(CB // LANES, CHUNKS)
    K = len(chunks)
    cfg = (Q, S, C, R, CB, chunks, local * n_clients * S)
    f32, bf16 = jnp.float32, jnp.bfloat16
    DMA = pltpu.SemaphoreType.DMA
    any_spec = pl.BlockSpec(memory_space=pl.ANY)
    blocks = rows // B
    vmem_spec = pl.BlockSpec(memory_space=pltpu.VMEM)
    new_rows, land = pl.pallas_call(
        functools.partial(kernel, cfg),
        out_shape=(pltpu.VMEM((2, 1, D), f32), pltpu.VMEM((2, blocks, B, D), bf16)),
        in_specs=[any_spec] * 6,
        out_specs=(vmem_spec,) * 2,
        scratch_shapes=[
            pltpu.VMEM((2, local, rows, D), bf16),
            pltpu.VMEM((local, rows, D), bf16),
            pltpu.VMEM((local, 8, LANES), f32),
            pltpu.VMEM((local, 8, LANES), f32),
            pltpu.VMEM((8, LANES), f32),
            pltpu.VMEM((8, LANES), f32),
            pltpu.VMEM((8, LANES), f32),
            pltpu.VMEM((Q - 1, 8, LANES), f32),
            pltpu.VMEM((S - 1, 8, LANES), f32),
            pltpu.VMEM((B, 1, CB), f32),
            pltpu.VMEM((Q, 2 * S, D), f32),
            pltpu.VMEM((Q - 1, 2 * S, D), f32),
            pltpu.VMEM((R, B, D), f32),
            pltpu.VMEM((S - 1, B, CB), f32),
            pltpu.VMEM((B, 1, CB), f32),
            pltpu.SMEM((local,), jnp.int32),
            pltpu.SMEM((local,), jnp.int32),
            DMA((4,)), DMA((2,)), DMA((2,)),
            DMA((Q - 1,)), DMA((Q - 1,)), DMA((S - 1,)), DMA((S - 1,)),
            DMA((2, C)), DMA((B,)),
            DMA((K, Q - 1)), DMA((K, Q - 1)), DMA((K, S - 1)), DMA((K, S - 1)),
            DMA((K, Q * S)), DMA((K, Q * S)), DMA((K, Q * S)), DMA((K, Q * S)),
            DMA((B, K)), DMA((2, C, K)),
        ],
        compiler_params=pltpu.CompilerParams(collective_id=0, has_side_effects=True),
    )(client_deltas, variate_deltas, params, variate, taking_part, counts)
    new_params, new_variate, cp, cv = pl.pallas_call(
        store_kernel,
        out_shape=(
            jax.ShapeDtypeStruct((1, D), f32),
            jax.ShapeDtypeStruct((1, D), f32),
            jax.ShapeDtypeStruct((blocks, B, D), bf16),
            jax.ShapeDtypeStruct((blocks, B, D), bf16),
        ),
        in_specs=[vmem_spec] * 2,
        out_specs=(any_spec,) * 4,
        scratch_shapes=[DMA((4,))],
    )(
        pltpu.with_memory_space_constraint(new_rows, pltpu.VMEM),
        pltpu.with_memory_space_constraint(land, pltpu.VMEM),
    )
    return new_params, new_variate, cp.reshape(rows, D), cv.reshape(rows, D)


def solution(mesh):
    both = ("clients", "shard")
    in_specs = (
        P(both, None, None),
        P(both, None, None),
        P(both, None),
        P(both, None),
        P(both),
        P(both),
    )
    out_specs = (P(both, None), P(both, None), P(), P())
    sizes = (mesh.shape["clients"], mesh.shape["shard"])
    return jax.shard_map(
        functools.partial(body, sizes),
        mesh=mesh, in_specs=in_specs, out_specs=out_specs, check_vma=False,
    )
```

```python
import functools
import math

import jax
import jax.numpy as jnp
from jax import lax
from jax.experimental import pallas as pl
from jax.experimental.pallas import tpu as pltpu
from jax.sharding import PartitionSpec as P

MESH = pl.DeviceIdType.MESH
LANES = 128
SHARES = (3, 4)
RELAYED = ((1, 2, 3), ())
UNROLL = True
FAR_FIRST = True


def split_blocks(blocks):
    out, at, seen = [], 0, 0
    for share in SHARES:
        seen += share
        end = blocks * seen // sum(SHARES)
        if end > at:
            out.append((at * LANES, (end - at) * LANES))
            at = end
    return out


def kernel(
    cfg,
    cd_ref, vd_ref, p_ref, v_ref, tp_ref, ct_ref,
    rows, land,
    mine, pair_send, pair_recv, w_send, w_recv, tot_a, tot_b, tot_c, tot_ra, tot_rb,
    prow, send1, recv1, send2, recv2, fin, tp_s, ct_s,
    in_sem, d2d_s, d2d_r, w1s, w1r, w2s, w2r, ps, pr, s1s, s1r, s2s, s2r,
    ags, agr, fws, fwr, os, osr,
):
    Q, S, C, R, CB, chunks, clients_total = cfg
    local = cd_ref.shape[0]
    cli = lax.axis_index("clients")
    s = lax.axis_index("shard")
    core = lax.rem(cli, 2)
    q = lax.div(cli, 2)
    other = 1 - core
    B = 2 * C
    sr, sc = lax.div(s, C), lax.rem(s, C)
    K = len(chunks)
    far = (lambda n: range(n - 1, 0, -1)) if FAR_FIRST else (lambda n: range(1, n))

    def dev(qq, cc, ss):
        return (qq * 2 + cc, ss)

    def rcopy(src, dst, ssem, rsem, device):
        return pltpu.make_async_remote_copy(
            src_ref=src, dst_ref=dst, send_sem=ssem, recv_sem=rsem,
            device_id=device, device_id_type=MESH,
        )

    loads = [
        pltpu.make_async_copy(cd_ref, mine.at[0], in_sem.at[0]),
        pltpu.make_async_copy(vd_ref, mine.at[1], in_sem.at[1]),
        pltpu.make_async_copy(tp_ref, tp_s, in_sem.at[2]),
        pltpu.make_async_copy(ct_ref, ct_s, in_sem.at[3]),
    ]
    for load in loads:
        load.start()

    barrier = pltpu.get_barrier_semaphore()
    greeted = 0
    for y in range(1, Q):
        greeted += 1
        pl.semaphore_signal(barrier, inc=1, device_id=dev(q ^ y, core, s), device_id_type=MESH)
    for x in range(S):
        for c in (core, other) if x else (other,):
            greeted += 1
            pl.semaphore_signal(barrier, inc=1, device_id=dev(q, c, s ^ x), device_id_type=MESH)

    loads[2].wait()
    loads[3].wait()
    here_w, there_w = [], []
    for i in range(local):
        took = tp_s[i]
        weighed = took * ct_s[i]
        here_w.append(jnp.where(core == 0, weighed, took).astype(jnp.float32))
        there_w.append(jnp.where(core == 0, took, weighed).astype(jnp.float32))
    w_send[...] = jnp.full((8, LANES), sum(there_w), jnp.float32)
    loads[0].wait()
    loads[1].wait()

    def chunk_cols(k):
        off, width = chunks[k]
        return slice(C * off, C * (off + width))

    def weigh(a, weights, cols):
        acc = None
        for i in range(local):
            term = mine[a, i, :, cols].astype(jnp.float32) * weights[i]
            acc = term if acc is None else acc + term
        return acc

    for k in range(len(chunks)):
        cols = chunk_cols(k)
        pair_send[:, cols] = weigh(other, there_w, cols)
        send1[:, :, cols] = weigh(core, here_w, cols).reshape(Q, 2 * S, -1)

    pl.semaphore_wait(barrier, greeted)

    partner = dev(q, other, s)
    w_copy = rcopy(w_send, w_recv, d2d_s.at[K], d2d_r.at[K], partner)
    w_copy.start()

    def pair_copy(k):
        cols = pl.ds(chunk_cols(k).start, C * chunks[k][1])
        return rcopy(
            pair_send.at[:, cols], pair_recv.at[:, cols], d2d_s.at[k], d2d_r.at[k], partner
        )

    for k in range(K):
        pair_copy(k).start()

    def piece_cols(c, k):
        off, width = chunks[k]
        return pl.ds(pl.multiple_of(C * off + c * width, LANES), width)

    jj = core * S + s
    j_block, j_in = lax.div(jj, B), lax.rem(jj, B)
    def base_copies():
        for a, src in enumerate((p_ref, v_ref)):
            for c in range(C):
                to_s = j_block * C + c
                me = jnp.logical_and(core == a, s == to_s)
                for k, (off, width) in enumerate(chunks):
                    piece = src.at[:, pl.ds(C * off + c * width, width)]
                    dst = prow.at[j_in, :, pl.ds(off, width)]
                    yield a, c, k, me, piece, dst, dev(q, a, to_s)

    for a, c, k, me, piece, dst, device in base_copies():
        @pl.when(me)
        def _():
            pltpu.make_async_copy(piece, dst, pr.at[j_in, k]).start()

        @pl.when(jnp.logical_not(me))
        def _():
            rcopy(piece, dst, ps.at[a, c, k], pr.at[j_in, k], device).start()

    w_copy.wait_recv()
    tot_a[...] = w_recv[...] + sum(here_w)

    def plane_copy(k, d):
        off, width = chunks[k]
        to_q = q ^ d
        return rcopy(
            send1.at[to_q, :, pl.ds(C * off, C * width)],
            recv1.at[d - 1, :, pl.ds(C * off, C * width)],
            s1s.at[k, d - 1], s1r.at[k, d - 1], dev(to_q, core, s),
        )

    def tot1_copy(d):
        return rcopy(
            tot_a, tot_ra.at[d - 1], w1s.at[d - 1], w1r.at[d - 1],
            dev(q ^ d, core, s),
        )

    def tot2_copy(e):
        return rcopy(
            tot_b, tot_rb.at[e - 1], w2s.at[e - 1], w2r.at[e - 1],
            dev(q, core, s ^ e),
        )

    for k in range(K):
        cols = chunk_cols(k)
        pair_copy(k).wait_recv()
        send1[:, :, cols] = send1[:, :, cols] + pair_recv[:, cols].reshape(Q, 2 * S, -1)
        if k == 0:
            for d in far(Q):
                tot1_copy(d).start()
        for d in far(Q):
            plane_copy(k, d).start()

    def shard_copy(k, e):
        off, width = chunks[k]
        to_s = s ^ e
        to_r, to_c = lax.div(to_s, C), lax.rem(to_s, C)
        return rcopy(
            send2.at[to_r, :, pl.ds(pl.multiple_of(C * off + to_c * width, LANES), width)],
            recv2.at[e - 1, :, pl.ds(off, width)],
            s2s.at[k, e - 1], s2r.at[k, e - 1], dev(q, core, to_s),
        )

    for k, (off, width) in enumerate(chunks):
        if k == 0:
            plane_weight = tot_a[...]
            for d in range(1, Q):
                tot1_copy(d).wait_recv()
                plane_weight = plane_weight + tot_ra[d - 1]
            tot_b[...] = plane_weight
        for d in range(1, Q):
            plane_copy(k, d).wait_recv()
        cols = slice(C * off, C * (off + width))
        acc = send1[q, :, cols]
        for d in range(1, Q):
            acc = acc + recv1[d - 1, :, cols]
        send2[:, :, cols] = acc.reshape(R, B, C * width)
        if k == 0:
            for e in range(1, S):
                tot2_copy(e).start()
        for e in far(S):
            shard_copy(k, e).start()

    block = q * R + sr

    def gather_copy(k, t):
        here = land.at[core, block, :, piece_cols(sc, k)]
        return rcopy(
            here, here, ags.at[k, t], agr.at[k, t], dev(q ^ (t // S), core, s ^ (t % S))
        )

    def source_ref(k, t, a):
        from_q, from_s = q ^ (t // S), s ^ (t % S)
        return land.at[
            a, from_q * R + lax.div(from_s, C), :, piece_cols(lax.rem(from_s, C), k)
        ]

    def each(first, act):
        if UNROLL and Q * S <= 16:
            for t in order():
                if t >= first:
                    act(t)
        else:
            pl.loop(first, Q * S)(act)

    def relayed(k):
        return [x for x in RELAYED[k] if x < S]

    def relay_copy(k, y, x):
        ref = source_ref(k, x, core)
        t = y * S + x
        return rcopy(ref, ref, ags.at[k, t], agr.at[k, t], dev(q ^ y, core, s))

    def is_direct(k, t):
        return t < S or t % S not in relayed(k)

    def each_direct(k, act):
        if relayed(k):
            for t in order():
                if t and is_direct(k, t):
                    act(t)
        else:
            each(1, act)

    def each_relay(k, act):
        for x in relayed(k):
            for y in range(Q - 1, 0, -1):
                act(y, x)

    def order():
        ts = [y * S + x for x in range(S - 1, -1, -1) for y in range(Q - 1, -1, -1)]
        return ts if FAR_FIRST else ts[::-1]

    def row_copy(k, j, src, device):
        dst = rows.at[core, :, piece_cols(sc, k)]
        return rcopy(src, dst, os.at[j, k], osr.at[core, sc, k], device)

    def forward_copy(k, t):
        ref = source_ref(k, t, core)
        return rcopy(ref, ref, fws.at[k, t], fwr.at[k, t], partner)

    def forward_recv(k, t):
        ref = source_ref(k, t, other)
        return rcopy(ref, ref, fws.at[k, t], fwr.at[k, t], partner)

    def row_targets(k):
        off, width = chunks[k]
        for j in range(B):
            row = sr * B + j
            to_core, to_s = lax.div(row, S), lax.rem(row, S)
            me = jnp.logical_and(to_core == core, to_s == s)
            yield j, me, dev(q, to_core, to_s), fin.at[j, :, pl.ds(off, width)]

    for k, (off, width) in enumerate(chunks):
        if k == 0:
            weight_total = tot_b[...]
            for e in range(1, S):
                tot2_copy(e).wait_recv()
                weight_total = weight_total + tot_rb[e - 1]
            tot_c[...] = jnp.where(core == 0, weight_total, jnp.float32(clients_total))
        for e in range(1, S):
            shard_copy(k, e).wait_recv()
        acc = send2[sr, :, pl.ds(pl.multiple_of(C * off + sc * width, LANES), width)]
        for e in range(1, S):
            acc = acc + recv2[e - 1, :, off:off + width]
        for j in range(B):
            pltpu.make_async_copy(
                p_ref.at[:, pl.ds(0, width)], prow.at[j, :, pl.ds(off, width)], pr.at[j, k]
            ).wait()
        base = jnp.concatenate([prow[j, :, off:off + width] for j in range(B)], axis=0)
        new = base + acc / tot_c[0:1, 0:1]
        land[core, block, :, piece_cols(sc, k)] = new.astype(jnp.bfloat16)
        for j in range(B):
            fin[j, :, off:off + width] = new[j:j + 1, :]

        each_direct(k, lambda t: gather_copy(k, t).start())
        forward_copy(k, 0).start()
        for j, me, device, src in row_targets(k):
            @pl.when(jnp.logical_not(me))
            def _():
                row_copy(k, j, src, device).start()

        @pl.when(j_block == sr)
        def _():
            rows[core, :, piece_cols(sc, k)] = fin[j_in, :, off:off + width]

    for k in range(K):
        for x in relayed(k):
            gather_copy(k, x).wait_recv()
            for y in range(Q - 1, 0, -1):
                relay_copy(k, y, x).start()
            forward_copy(k, x).start()

    w_copy.wait_send()
    for a, c, k, me, piece, dst, device in base_copies():
        @pl.when(jnp.logical_not(me))
        def _():
            rcopy(piece, dst, ps.at[a, c, k], pr.at[j_in, k], device).wait_send()
    for d in range(1, Q):
        tot1_copy(d).wait_send()
    for e in range(1, S):
        tot2_copy(e).wait_send()
    for k in range(K):
        pair_copy(k).wait_send()
        for d in range(1, Q):
            plane_copy(k, d).wait_send()
        for e in range(1, S):
            shard_copy(k, e).wait_send()

    for k in range(K):
        def pass_on(t):
            gather_copy(k, t).wait_recv()
            forward_copy(k, t).start()

        if relayed(k):
            for t in order():
                if t >= S or (t and t not in relayed(k)):
                    pass_on(t)
        else:
            each(1, pass_on)

    for k in range(K):
        each_direct(k, lambda t: gather_copy(k, t).wait_send())
        each_relay(k, lambda y, x: relay_copy(k, y, x).wait_send())
        for j, me, device, src in row_targets(k):
            @pl.when(jnp.logical_not(me))
            def _():
                row_copy(k, j, src, device).wait_send()
    for k in range(K):
        each(0, lambda t: forward_recv(k, t).wait_recv())

    for k, (off, width) in enumerate(chunks):
        each(0, lambda t: forward_copy(k, t).wait_send())
        for a in range(2):
            for c in range(C):
                me = jnp.logical_and(core == a, s == j_block * C + c)

                @pl.when(jnp.logical_not(me))
                def _():
                    rcopy(
                        fin.at[0, :, pl.ds(off, width)], rows.at[a, :, piece_cols(c, k)],
                        os.at[0, k], osr.at[a, c, k], partner,
                    ).wait_recv()


def store_kernel(rows, land, np_ref, nv_ref, cp_ref, cv_ref, sem):
    copies = [
        pltpu.make_async_copy(land.at[0], cp_ref, sem.at[0]),
        pltpu.make_async_copy(land.at[1], cv_ref, sem.at[1]),
        pltpu.make_async_copy(rows.at[0], np_ref, sem.at[2]),
        pltpu.make_async_copy(rows.at[1], nv_ref, sem.at[3]),
    ]
    for copy in copies:
        copy.start()
    for copy in copies:
        copy.wait()


def body(sizes, client_deltas, variate_deltas, params, variate, taking_part, counts):
    n_clients, S = sizes
    Q = n_clients // 2
    local, rows, D = client_deltas.shape
    C = math.gcd(S, D // LANES)
    R = S // C
    B = 2 * C
    CB = D // C
    chunks = split_blocks(CB // LANES)
    K = len(chunks)
    cfg = (Q, S, C, R, CB, chunks, local * n_clients * S)
    f32, bf16 = jnp.float32, jnp.bfloat16
    DMA = pltpu.SemaphoreType.DMA
    any_spec = pl.BlockSpec(memory_space=pl.ANY)
    blocks = rows // B
    vmem_spec = pl.BlockSpec(memory_space=pltpu.VMEM)
    new_rows, land = pl.pallas_call(
        functools.partial(kernel, cfg),
        out_shape=(pltpu.VMEM((2, 1, D), f32), pltpu.VMEM((2, blocks, B, D), bf16)),
        in_specs=[any_spec] * 6,
        out_specs=(vmem_spec,) * 2,
        scratch_shapes=[
            pltpu.VMEM((2, local, rows, D), bf16),
            pltpu.VMEM((rows, D), f32),
            pltpu.VMEM((rows, D), f32),
            pltpu.VMEM((8, LANES), f32),
            pltpu.VMEM((8, LANES), f32),
            pltpu.VMEM((8, LANES), f32),
            pltpu.VMEM((8, LANES), f32),
            pltpu.VMEM((8, LANES), f32),
            pltpu.VMEM((Q - 1, 8, LANES), f32),
            pltpu.VMEM((S - 1, 8, LANES), f32),
            pltpu.VMEM((B, 1, CB), f32),
            pltpu.VMEM((Q, 2 * S, D), f32),
            pltpu.VMEM((Q - 1, 2 * S, D), f32),
            pltpu.VMEM((R, B, D), f32),
            pltpu.VMEM((S - 1, B, CB), f32),
            pltpu.VMEM((B, 1, CB), f32),
            pltpu.SMEM((local,), jnp.int32),
            pltpu.SMEM((local,), jnp.int32),
            DMA((4,)), DMA((K + 1,)), DMA((K + 1,)),
            DMA((Q - 1,)), DMA((Q - 1,)), DMA((S - 1,)), DMA((S - 1,)),
            DMA((2, C, K)), DMA((B, K)),
            DMA((K, Q - 1)), DMA((K, Q - 1)), DMA((K, S - 1)), DMA((K, S - 1)),
            DMA((K, Q * S)), DMA((K, Q * S)), DMA((K, Q * S)), DMA((K, Q * S)),
            DMA((B, K)), DMA((2, C, K)),
        ],
        compiler_params=pltpu.CompilerParams(collective_id=0, has_side_effects=True),
    )(client_deltas, variate_deltas, params, variate, taking_part, counts)
    new_params, new_variate, cp, cv = pl.pallas_call(
        store_kernel,
        out_shape=(
            jax.ShapeDtypeStruct((1, D), f32),
            jax.ShapeDtypeStruct((1, D), f32),
            jax.ShapeDtypeStruct((blocks, B, D), bf16),
            jax.ShapeDtypeStruct((blocks, B, D), bf16),
        ),
        in_specs=[vmem_spec] * 2,
        out_specs=(any_spec,) * 4,
        scratch_shapes=[DMA((4,))],
    )(
        pltpu.with_memory_space_constraint(new_rows, pltpu.VMEM),
        pltpu.with_memory_space_constraint(land, pltpu.VMEM),
    )
    return new_params, new_variate, cp.reshape(rows, D), cv.reshape(rows, D)


def solution(mesh):
    both = ("clients", "shard")
    in_specs = (
        P(both, None, None),
        P(both, None, None),
        P(both, None),
        P(both, None),
        P(both),
        P(both),
    )
    out_specs = (P(both, None), P(both, None), P(), P())
    sizes = (mesh.shape["clients"], mesh.shape["shard"])
    return jax.shard_map(
        functools.partial(body, sizes),
        mesh=mesh, in_specs=in_specs, out_specs=out_specs, check_vma=False,
    )
```
